32 devices in a mesh: time: 8 (over y, x, core), chan: 4 (over z).
Axes of the slice: x: 2, y: 2, z: 4, core: 2. Of those that a mesh axis runs over, the one named last changes fastest.
Arguments:
- decay_rate: float32 [4, 4096, 2560], P(None, 'time', 'chan'), may hold values from 0.2 to 2
- drive_in: bfloat16 [4, 4096, 2560], P(None, 'time', 'chan'), may hold values from -6 to 6
- gate_in: bfloat16 [4, 4096, 2560], P(None, 'time', 'chan'), may hold values from -6 to 6
- norm_gain: float32 [2560], P('chan'), may hold values from 0.25 to 1.75
Outputs:
- filtered: bfloat16 [4, 4096, 2560], P(None, 'time', 'chan')
The draws below stay inside these ranges and needn't reach their ends.
All inputs are finite; a program needn't handle non-finite values.
Results may differ from the reference program's by a relative error of at most 0.0015.
Values sent between devices are 32-bit elements.
A program may use at most 128 MiB of HBM per device.

```python
import jax
import jax.numpy as jnp
from jax import lax

BATCH = 4
CHANNELS = 2560
LENGTH = 4096


def levels(rng, extent, cuts, least, largest):
    level = 1.0
    for position, shards_of in cuts:
        steps = jax.random.uniform(jax.random.fold_in(jax.random.fold_in(rng, 6), position), (shards_of,), jnp.float32, least / len(cuts), largest / len(cuts))
        level = level * jnp.repeat(jnp.exp(steps), extent[position] // shards_of).reshape((-1,) + (1,) * (len(extent) - 1 - position))
    return level


def bell_draw(key, dims, scale, limit, pieces=(), kind=jnp.bfloat16):
    array = scale * jax.random.normal(key, dims, jnp.float32)
    if pieces:
        array = array * levels(key, dims, pieces, -0.22, 0.18)
    return jnp.clip(array, -limit, limit).astype(kind)


def setup_inputs(seed: int = 0) -> dict:
    arg_keys = jax.random.split(jax.random.key(seed), 5)
    return {
        "decay_rate": jnp.clip(0.2 + 1.8 * jax.random.uniform(arg_keys[0], (BATCH, LENGTH, CHANNELS), jnp.float32) ** levels(arg_keys[0], (BATCH, LENGTH, CHANNELS), ((1, 8), (2, 4)), -0.2, 0.2), 0.2, 2.0),
        "drive_in": bell_draw(arg_keys[1], (BATCH, LENGTH, CHANNELS), 1.0, 6.0, ((1, 8), (2, 4))),
        "gate_in": bell_draw(arg_keys[2], (BATCH, LENGTH, CHANNELS), 1.0, 6.0, ((1, 8), (2, 4))),
        "norm_gain": jnp.clip(1.0 + 0.15 * jax.random.normal(arg_keys[3], (CHANNELS,), jnp.float32), 0.25, 1.75),
    }


def join_pair(earlier, later):
    return (earlier[0] * later[0], later[0] * earlier[1] + later[1])

def reference(decay_rate, drive_in, gate_in, norm_gain):
    keep = jnp.exp(-decay_rate / LENGTH)
    push = drive_in.astype(jnp.float32) * LENGTH ** (-0.5)
    forward = lax.associative_scan(join_pair, (keep, push), axis=1)[1]
    gated = forward * jax.nn.sigmoid(gate_in.astype(jnp.float32))
    power = lax.optimization_barrier(jnp.mean(gated * gated, axis=-1, keepdims=True))
    filtered = (gated * lax.rsqrt(power + 1e-06) * norm_gain).astype(jnp.bfloat16)
    return filtered
```

```python
import functools
import math

import jax
import jax.numpy as jnp
from jax import lax
from jax.experimental import pallas as pl
from jax.experimental.pallas import tpu as pltpu
from jax.sharding import PartitionSpec as P

BLOCK = 128
LANES = 128
MESH = pl.DeviceIdType.MESH


def split(x):
    hi = x.astype(jnp.bfloat16)
    lo = (x - hi.astype(jnp.float32)).astype(jnp.bfloat16)
    return jnp.concatenate([hi, lo], axis=0)


def kernel(times, chans, dec_hbm, drv_hbm, gate_hbm, gain_ref, tri_ref, out_hbm,
           dec, drv, gate, run, outb, keeps, sums, mine, theirs, power, powers,
           in_sem, out_sem, t_send, t_recv, c_send, c_recv):
    batch, length, width = dec.shape
    blocks = length // BLOCK
    total = length * times
    rate = math.log2(math.e) / total
    scale = 0.5 * total ** -0.5
    t, c = lax.axis_index("time"), lax.axis_index("chan")

    places = ((dec_hbm, dec), (drv_hbm, drv), (gate_hbm, gate))

    def load(i, b):
        return pltpu.make_async_copy(places[i][0].at[b], places[i][1].at[b], in_sem.at[i, b])

    def store(b):
        return pltpu.make_async_copy(outb.at[b], out_hbm.at[b], out_sem.at[b])

    def time_copy(b, peer):
        return pltpu.make_async_remote_copy(
            src_ref=mine.at[b], dst_ref=theirs.at[b, t], send_sem=t_send.at[b, peer],
            recv_sem=t_recv.at[b, t], device_id={"time": peer}, device_id_type=MESH)

    def time_arrival(b, peer):
        return pltpu.make_async_remote_copy(
            src_ref=mine.at[b], dst_ref=theirs.at[b, peer], send_sem=t_send.at[b, peer],
            recv_sem=t_recv.at[b, peer], device_id={"time": peer}, device_id_type=MESH)

    def chan_copy(b, step):
        return pltpu.make_async_remote_copy(
            src_ref=power.at[b], dst_ref=powers.at[b, step - 1], send_sem=c_send.at[b, step - 1],
            recv_sem=c_recv.at[b, step - 1], device_id={"chan": lax.rem(c + step, chans)},
            device_id_type=MESH)

    for b in range(batch):
        load(0, b).start()
        load(1, b).start()
    for b in range(batch):
        load(2, b).start()

    barrier = pltpu.get_barrier_semaphore()
    for step in range(1, times):
        pl.semaphore_signal(barrier, inc=1, device_id={"time": lax.rem(t + step, times)},
                            device_id_type=MESH)
    for step in range(1, chans):
        pl.semaphore_signal(barrier, inc=1, device_id={"chan": lax.rem(c + step, chans)},
                            device_id_type=MESH)

    def rows(k):
        return pl.ds(pl.multiple_of(k * BLOCK, BLOCK), BLOCK)

    def first(b):
        load(0, b).wait()
        load(1, b).wait()

        def block(k, carried):
            kept, state = carried
            at = rows(k)
            so_far = rate * jnp.dot(tri_ref[...], split(dec[b, at, :]),
                                    preferred_element_type=jnp.float32)
            entered = jnp.exp2(so_far) * drv[b, at, :].astype(jnp.float32)
            dec[b, at, :] = so_far
            run[b, at, :] = entered
            keep = jnp.exp2(-so_far[BLOCK - 1:, :])
            gained = jnp.sum(entered, axis=0, keepdims=True)
            keeps[b, k] = keep
            sums[b, k] = gained
            return kept * keep, keep * (state + gained)

        kept, state = lax.fori_loop(
            0, blocks, block, (jnp.ones((1, width), jnp.float32), jnp.zeros((1, width), jnp.float32)))
        mine[b, 0:1, :] = kept
        mine[b, 1:2, :] = state

    def send_times(b):
        def send(peer, _):
            time_copy(b, peer).start()
            return 0
        lax.fori_loop(t + 1, times, send, 0)

    first(0)
    pl.semaphore_wait(barrier, times + chans - 2)
    send_times(0)

    def more(b, _):
        first(b)
        send_times(b)
        return 0
    lax.fori_loop(1, batch, more, 0)

    def second(b, _):
        load(2, b).wait()

        def block(k, _):
            at = rows(k)
            opened = 1.0 + jnp.tanh(0.5 * gate[b, at, :].astype(jnp.float32))
            dec[b, at, :] = jnp.exp2(-dec[b, at, :]) * opened
            run[b, at, :] = jnp.dot(tri_ref[...], split(run[b, at, :]),
                                    preferred_element_type=jnp.float32)
            return 0
        lax.fori_loop(0, blocks, block, 0)
        return 0
    lax.fori_loop(0, batch, second, 0)

    def third(b, _):
        def arrive(peer, state):
            time_arrival(b, peer).wait_recv()
            return theirs[b, peer, 0:1, :] * state + theirs[b, peer, 1:2, :]
        state = lax.fori_loop(0, t, arrive, jnp.zeros((1, width), jnp.float32))

        def block(k, state):
            at = rows(k)
            gated = dec[b, at, :] * (run[b, at, :] + state)
            run[b, at, :] = gated
            squares = gated * gated
            folded = squares[:, :LANES]
            for lane in range(LANES, width, LANES):
                folded = folded + squares[:, lane:lane + LANES]
            power[b, pl.ds(k, 1), :] = lax.dot_general(
                jnp.ones((8, LANES), jnp.float32), folded, (((1,), (1,)), ((), ())),
                precision=lax.Precision.HIGHEST, preferred_element_type=jnp.float32)[0:1]
            return keeps[b, k] * (state + sums[b, k])
        lax.fori_loop(0, blocks, block, state)
        for step in range(1, chans):
            chan_copy(b, step).start()
        return 0
    lax.fori_loop(0, batch, third, 0)

    def fourth(b, _):
        mean = power[b]
        for step in range(1, chans):
            chan_copy(b, step).wait_recv()
            mean = mean + powers[b, step - 1]
        mean = mean * (scale * scale / (width * chans))
        factor = scale * lax.rsqrt(mean + 1e-6)
        gain = gain_ref[...]
        for k in range(blocks):
            at = pl.ds(k * BLOCK, BLOCK)
            tall = jnp.transpose(jnp.broadcast_to(factor[k:k + 1, :], (LANES, BLOCK)))
            for lane in range(0, width, LANES):
                cut = pl.ds(lane, LANES)
                outb[b, at, cut] = (run[b, at, cut] * tall * gain[:, lane:lane + LANES]).astype(outb.dtype)
        store(b).start()
        return 0
    lax.fori_loop(0, batch, fourth, 0)

    def finish(b, _):
        def sent(peer, _):
            time_copy(b, peer).wait_send()
            return 0
        lax.fori_loop(t + 1, times, sent, 0)
        for step in range(1, chans):
            chan_copy(b, step).wait_send()
        store(b).wait()
        return 0
    lax.fori_loop(0, batch, finish, 0)


def shards(decay_rate, drive_in, gate_in, norm_gain):
    times, chans = lax.axis_size("time"), lax.axis_size("chan")
    batch, length, width = decay_rate.shape
    blocks = length // BLOCK
    lower = jnp.tril(jnp.ones((BLOCK, BLOCK), jnp.bfloat16))
    any_space = pl.BlockSpec(memory_space=pl.ANY)
    vmem = pl.BlockSpec(memory_space=pltpu.VMEM)
    dma = pltpu.SemaphoreType.DMA
    f32 = jnp.float32
    return pl.pallas_call(
        functools.partial(kernel, times, chans),
        out_shape=jax.ShapeDtypeStruct(decay_rate.shape, jnp.bfloat16),
        in_specs=[any_space] * 3 + [vmem] * 2,
        out_specs=any_space,
        scratch_shapes=[
            pltpu.VMEM((batch, length, width), f32),
            pltpu.VMEM((batch, length, width), drive_in.dtype),
            pltpu.VMEM((batch, length, width), gate_in.dtype),
            pltpu.VMEM((batch, length, width), f32),
            pltpu.VMEM((batch, length, width), jnp.bfloat16),
            pltpu.VMEM((batch, blocks, 1, width), f32),
            pltpu.VMEM((batch, blocks, 1, width), f32),
            pltpu.VMEM((batch, 2, width), f32),
            pltpu.VMEM((batch, times, 2, width), f32),
            pltpu.VMEM((batch, blocks, BLOCK), f32),
            pltpu.VMEM((batch, chans - 1, blocks, BLOCK), f32),
            dma((3, batch)),
            dma((batch,)),
            dma((batch, times)),
            dma((batch, times)),
            dma((batch, chans - 1)),
            dma((batch, chans - 1)),
        ],
        compiler_params=pltpu.CompilerParams(
            collective_id=0, has_side_effects=True, vmem_limit_bytes=60 * 2 ** 20),
    )(decay_rate, drive_in, gate_in, norm_gain.reshape(1, width), jnp.concatenate([lower, lower], axis=1))


def solution(mesh):
    placed = (P(None, "time", "chan"), P(None, "time", "chan"), P(None, "time", "chan"), P("chan"))
    return jax.shard_map(
        shards, mesh=mesh, in_specs=placed, out_specs=P(None, "time", "chan"), check_vma=False
    )
```

```python
import functools
import math

import jax
import jax.numpy as jnp
from jax import lax
from jax.experimental import pallas as pl
from jax.experimental.pallas import tpu as pltpu
from jax.sharding import PartitionSpec as P

BLOCK = 128
LANES = 128
MESH = pl.DeviceIdType.MESH


def split(x):
    hi = x.astype(jnp.bfloat16)
    lo = (x - hi.astype(jnp.float32)).astype(jnp.bfloat16)
    return jnp.concatenate([hi, lo], axis=0)


def kernel(times, chans, dec_hbm, drv_hbm, gate_hbm, gain_ref, outb,
           tri_ref, dec, drv, gate, run, keeps, sums, mine, theirs, power, powers,
           in_sem, t_send, t_recv, c_send, c_recv):
    batch, length, width = dec.shape
    blocks = length // BLOCK
    total = length * times
    rate = math.log2(math.e) / total
    scale = 0.5 * total ** -0.5
    t, c = lax.axis_index("time"), lax.axis_index("chan")

    places = ((dec_hbm, dec), (drv_hbm, drv), (gate_hbm, gate))

    def load(i, b):
        return pltpu.make_async_copy(places[i][0].at[b], places[i][1].at[b], in_sem.at[i, b])

    def time_copy(b, peer):
        return pltpu.make_async_remote_copy(
            src_ref=mine.at[b], dst_ref=theirs.at[b, t], send_sem=t_send.at[b, peer],
            recv_sem=t_recv.at[b, t], device_id={"time": peer}, device_id_type=MESH)

    def time_arrival(b, peer):
        return pltpu.make_async_remote_copy(
            src_ref=mine.at[b], dst_ref=theirs.at[b, peer], send_sem=t_send.at[b, peer],
            recv_sem=t_recv.at[b, peer], device_id={"time": peer}, device_id_type=MESH)

    def chan_copy(b, step):
        return pltpu.make_async_remote_copy(
            src_ref=power.at[b], dst_ref=powers.at[b, step - 1], send_sem=c_send.at[b, step - 1],
            recv_sem=c_recv.at[b, step - 1], device_id={"chan": lax.rem(c + step, chans)},
            device_id_type=MESH)

    for b in range(batch):
        load(0, b).start()
        load(1, b).start()
    for b in range(batch):
        load(2, b).start()

    barrier = pltpu.get_barrier_semaphore()
    for step in range(1, times):
        pl.semaphore_signal(barrier, inc=1, device_id={"time": lax.rem(t + step, times)},
                            device_id_type=MESH)
    for step in range(1, chans):
        pl.semaphore_signal(barrier, inc=1, device_id={"chan": lax.rem(c + step, chans)},
                            device_id_type=MESH)

    below = lax.broadcasted_iota(jnp.int32, (BLOCK, BLOCK), 0) >= lax.broadcasted_iota(
        jnp.int32, (BLOCK, BLOCK), 1)
    lower = jnp.where(below, 1.0, 0.0).astype(jnp.bfloat16)
    tri_ref[:, :BLOCK] = lower
    tri_ref[:, BLOCK:] = lower

    def rows(k):
        return pl.ds(pl.multiple_of(k * BLOCK, BLOCK), BLOCK)

    def first(b):
        load(0, b).wait()
        load(1, b).wait()

        def block(k, carried):
            kept, state = carried
            at = rows(k)
            so_far = rate * jnp.dot(tri_ref[...], split(dec[b, at, :]),
                                    preferred_element_type=jnp.float32)
            entered = jnp.exp2(so_far) * drv[b, at, :].astype(jnp.float32)
            dec[b, at, :] = so_far
            run[b, at, :] = entered
            keep = jnp.exp2(-so_far[BLOCK - 1:, :])
            gained = jnp.sum(entered, axis=0, keepdims=True)
            keeps[b, k] = keep
            sums[b, k] = gained
            return kept * keep, keep * (state + gained)

        kept, state = lax.fori_loop(
            0, blocks, block, (jnp.ones((1, width), jnp.float32), jnp.zeros((1, width), jnp.float32)))
        mine[b, 0:1, :] = kept
        mine[b, 1:2, :] = state

    def send_times(b):
        def send(peer, _):
            time_copy(b, peer).start()
            return 0
        lax.fori_loop(t + 1, times, send, 0)

    first(0)
    pl.semaphore_wait(barrier, times + chans - 2)
    send_times(0)

    def more(b, _):
        first(b)
        send_times(b)
        return 0
    lax.fori_loop(1, batch, more, 0)

    def second(b, _):
        load(2, b).wait()

        def block(k, _):
            at = rows(k)
            opened = 1.0 + jnp.tanh(0.5 * gate[b, at, :].astype(jnp.float32))
            dec[b, at, :] = jnp.exp2(-dec[b, at, :]) * opened
            run[b, at, :] = jnp.dot(tri_ref[...], split(run[b, at, :]),
                                    preferred_element_type=jnp.float32)
            return 0
        lax.fori_loop(0, blocks, block, 0)
        return 0
    lax.fori_loop(0, batch, second, 0)

    def third(b, _):
        def arrive(peer, state):
            time_arrival(b, peer).wait_recv()
            return theirs[b, peer, 0:1, :] * state + theirs[b, peer, 1:2, :]
        state = lax.fori_loop(0, t, arrive, jnp.zeros((1, width), jnp.float32))

        def block(k, state):
            at = rows(k)
            gated = dec[b, at, :] * (run[b, at, :] + state)
            run[b, at, :] = gated
            squares = gated * gated
            folded = squares[:, :LANES]
            for lane in range(LANES, width, LANES):
                folded = folded + squares[:, lane:lane + LANES]
            power[b, pl.ds(k, 1), :] = lax.dot_general(
                jnp.ones((8, LANES), jnp.float32), folded, (((1,), (1,)), ((), ())),
                precision=lax.Precision.HIGHEST, preferred_element_type=jnp.float32)[0:1]
            return keeps[b, k] * (state + sums[b, k])
        lax.fori_loop(0, blocks, block, state)
        for step in range(1, chans):
            chan_copy(b, step).start()
        return 0
    lax.fori_loop(0, batch, third, 0)

    def fourth(b, _):
        mean = power[b]
        for step in range(1, chans):
            chan_copy(b, step).wait_recv()
            mean = mean + powers[b, step - 1]
        mean = mean * (scale * scale / (width * chans))
        factor = scale * lax.rsqrt(mean + 1e-6)
        gain = gain_ref[...].reshape(1, width)
        for k in range(blocks):
            at = pl.ds(k * BLOCK, BLOCK)
            tall = jnp.transpose(jnp.broadcast_to(factor[k:k + 1, :], (LANES, BLOCK)))
            for lane in range(0, width, LANES):
                cut = pl.ds(lane, LANES)
                outb[b, at, cut] = (run[b, at, cut] * tall * gain[:, lane:lane + LANES]).astype(outb.dtype)
        return 0
    lax.fori_loop(0, batch, fourth, 0)

    def finish(b, _):
        def sent(peer, _):
            time_copy(b, peer).wait_send()
            return 0
        lax.fori_loop(t + 1, times, sent, 0)
        for step in range(1, chans):
            chan_copy(b, step).wait_send()
        return 0
    lax.fori_loop(0, batch, finish, 0)


def shards(decay_rate, drive_in, gate_in, norm_gain):
    times, chans = lax.axis_size("time"), lax.axis_size("chan")
    batch, length, width = decay_rate.shape
    blocks = length // BLOCK
    any_space = pl.BlockSpec(memory_space=pl.ANY)
    vmem = pl.BlockSpec(memory_space=pltpu.VMEM)
    dma = pltpu.SemaphoreType.DMA
    f32 = jnp.float32
    return pl.pallas_call(
        functools.partial(kernel, times, chans),
        out_shape=pltpu.VMEM(decay_rate.shape, jnp.bfloat16),
        in_specs=[any_space] * 3 + [vmem],
        out_specs=vmem,
        scratch_shapes=[
            pltpu.VMEM((BLOCK, 2 * BLOCK), jnp.bfloat16),
            pltpu.VMEM((batch, length, width), f32),
            pltpu.VMEM((batch, length, width), drive_in.dtype),
            pltpu.VMEM((batch, length, width), gate_in.dtype),
            pltpu.VMEM((batch, length, width), f32),
            pltpu.VMEM((batch, blocks, 1, width), f32),
            pltpu.VMEM((batch, blocks, 1, width), f32),
            pltpu.VMEM((batch, 2, width), f32),
            pltpu.VMEM((batch, times, 2, width), f32),
            pltpu.VMEM((batch, blocks, BLOCK), f32),
            pltpu.VMEM((batch, chans - 1, blocks, BLOCK), f32),
            dma((3, batch)),
            dma((batch, times)),
            dma((batch, times)),
            dma((batch, chans - 1)),
            dma((batch, chans - 1)),
        ],
        compiler_params=pltpu.CompilerParams(
            collective_id=0, has_side_effects=True, vmem_limit_bytes=58 * 2 ** 20),
    )(decay_rate, drive_in, gate_in, norm_gain)


def solution(mesh):
    placed = (P(None, "time", "chan"), P(None, "time", "chan"), P(None, "time", "chan"), P("chan"))
    return jax.shard_map(
        shards, mesh=mesh, in_specs=placed, out_specs=P(None, "time", "chan"), check_vma=False
    )
```

```python
import functools
import math

import jax
import jax.numpy as jnp
from jax import lax
from jax.experimental import pallas as pl
from jax.experimental.pallas import tpu as pltpu
from jax.sharding import PartitionSpec as P

BLOCK = 128
LANES = 128
PIECE = 64
MESH = pl.DeviceIdType.MESH


def split(x):
    hi = x.astype(jnp.bfloat16)
    lo = (x - hi.astype(jnp.float32)).astype(jnp.bfloat16)
    return jnp.concatenate([hi, lo], axis=0)


def kernel(times, chans, dec_hbm, drv_hbm, gate_hbm, gain_hbm, outb,
           gain_ref, tri_ref, dec, drv, gate, run, keeps, sums, mine, theirs, folds, power, powers,
           in_sem, head_sem, gain_sem, t_send, t_recv, c_send, c_recv):
    batch, length, width = dec.shape
    blocks = length // BLOCK
    total = length * times
    rate = math.log2(math.e) / total
    scale = 0.5 * total ** -0.5
    t, c = lax.axis_index("time"), lax.axis_index("chan")

    places = ((dec_hbm, dec), (drv_hbm, drv), (gate_hbm, gate))

    def load(i, b):
        return pltpu.make_async_copy(places[i][0].at[b], places[i][1].at[b], in_sem.at[i, b])

    def time_copy(b, peer):
        return pltpu.make_async_remote_copy(
            src_ref=mine.at[b], dst_ref=theirs.at[b, t], send_sem=t_send.at[b, peer],
            recv_sem=t_recv.at[b, t], device_id={"time": peer}, device_id_type=MESH)

    def time_arrival(b, peer):
        return pltpu.make_async_remote_copy(
            src_ref=mine.at[b], dst_ref=theirs.at[b, peer], send_sem=t_send.at[b, peer],
            recv_sem=t_recv.at[b, peer], device_id={"time": peer}, device_id_type=MESH)

    def chan_copy(b, step):
        return pltpu.make_async_remote_copy(
            src_ref=power.at[b], dst_ref=powers.at[b, step - 1], send_sem=c_send.at[b, step - 1],
            recv_sem=c_recv.at[b, step - 1], device_id={"chan": lax.rem(c + step, chans)},
            device_id_type=MESH)

    def head(i, k):
        at = pl.ds(k * BLOCK, BLOCK)
        return pltpu.make_async_copy(
            places[i][0].at[0, at], places[i][1].at[0, at], head_sem.at[i, k])

    for k in range(blocks):
        head(0, k).start()
        head(1, k).start()
    if batch > 1:
        load(0, 1).start()
        load(1, 1).start()

    barrier = pltpu.get_barrier_semaphore()
    for step in range(1, times):
        pl.semaphore_signal(barrier, inc=1, device_id={"time": lax.rem(t + step, times)},
                            device_id_type=MESH)
    for step in range(1, chans):
        pl.semaphore_signal(barrier, inc=1, device_id={"chan": lax.rem(c + step, chans)},
                            device_id_type=MESH)

    below = lax.broadcasted_iota(jnp.int32, (BLOCK, BLOCK), 0) >= lax.broadcasted_iota(
        jnp.int32, (BLOCK, BLOCK), 1)
    lower = jnp.where(below, 1.0, 0.0).astype(jnp.bfloat16)
    tri_ref[:, :BLOCK] = lower
    tri_ref[:, BLOCK:] = lower

    def rows(k):
        return pl.ds(pl.multiple_of(k * BLOCK, BLOCK), BLOCK)

    def first(b, early):
        if not early:
            load(0, b).wait()
            load(1, b).wait()

        def block(k, carried):
            if early:
                head(0, k).wait()
                head(1, k).wait()
            kept, state = carried
            at = rows(k)
            so_far = rate * jnp.dot(tri_ref[...], split(dec[b, at, :]),
                                    preferred_element_type=jnp.float32)
            entered = jnp.exp2(so_far) * drv[b, at, :].astype(jnp.float32)
            dec[b, at, :] = so_far
            run[b, at, :] = entered
            keep = jnp.exp2(-so_far[BLOCK - 1:, :])
            gained = jnp.sum(entered, axis=0, keepdims=True)
            keeps[b, k] = keep
            sums[b, k] = gained
            return kept * keep, keep * (state + gained)

        kept, state = lax.fori_loop(
            0, blocks, block, (jnp.ones((1, width), jnp.float32), jnp.zeros((1, width), jnp.float32)))
        mine[b, 0:1, :] = kept
        mine[b, 1:2, :] = state

    def send_times(b):
        def send(peer, _):
            time_copy(b, peer).start()
            return 0
        lax.fori_loop(t + 1, times, send, 0)

    for b in range(2, batch):
        load(0, b).start()
        load(1, b).start()
    first(0, True)
    for b in range(batch):
        load(2, b).start()
    gain_copy = pltpu.make_async_copy(gain_hbm, gain_ref, gain_sem)
    gain_copy.start()
    pl.semaphore_wait(barrier, times + chans - 2)
    send_times(0)

    def more(b, _):
        first(b, False)
        send_times(b)
        return 0
    lax.fori_loop(1, batch, more, 0)

    def second(b):
        load(2, b).wait()

        def opening(k, _):
            at = pl.ds(pl.multiple_of(k * PIECE, PIECE), PIECE)
            opened = 1.0 + jnp.tanh(0.5 * gate[b, at, :].astype(jnp.float32))
            dec[b, at, :] = jnp.exp2(-dec[b, at, :]) * opened
            return 0
        lax.fori_loop(0, length // PIECE, opening, 0)

        def block(k, _):
            at = rows(k)
            run[b, at, :] = jnp.dot(tri_ref[...], split(run[b, at, :]),
                                    preferred_element_type=jnp.float32)
            return 0
        lax.fori_loop(0, blocks, block, 0)

    def third(b):
        def arrive(peer, state):
            time_arrival(b, peer).wait_recv()
            return theirs[b, peer, 0:1, :] * state + theirs[b, peer, 1:2, :]
        state = lax.fori_loop(0, t, arrive, jnp.zeros((1, width), jnp.float32))

        def block(k, state):
            at = rows(k)
            gated = dec[b, at, :] * (run[b, at, :] + state)
            run[b, at, :] = gated
            squares = gated * gated
            folded = squares[:, :LANES]
            for lane in range(LANES, width, LANES):
                folded = folded + squares[:, lane:lane + LANES]
            hi = folded.astype(jnp.bfloat16)
            folds[at, :LANES] = hi
            folds[at, LANES:] = (folded - hi.astype(jnp.float32)).astype(jnp.bfloat16)
            return keeps[b, k] * (state + sums[b, k])
        lax.fori_loop(0, blocks, block, state)
        power[b] = lax.dot_general(
            jnp.ones((8, 2 * LANES), jnp.bfloat16), folds[...], (((1,), (1,)), ((), ())),
            preferred_element_type=jnp.float32)[0:1]
        for step in range(1, chans):
            chan_copy(b, step).start()

    second(0)

    def middle(b, _):
        second(b)
        third(b - 1)
        return 0
    lax.fori_loop(1, batch, middle, 0)
    third(batch - 1)
    gain_copy.wait()

    def fourth(b, _):
        mean = power[b]
        for step in range(1, chans):
            chan_copy(b, step).wait_recv()
            mean = mean + powers[b, step - 1]
        mean = mean * (scale * scale / (width * chans))
        factor = scale * lax.rsqrt(mean + 1e-6)
        gain = gain_ref[...].reshape(1, width)
        for k in range(blocks):
            at = pl.ds(k * BLOCK, BLOCK)
            tall = jnp.transpose(jnp.broadcast_to(factor[:, k * BLOCK:(k + 1) * BLOCK], (LANES, BLOCK)))
            for lane in range(0, width, LANES):
                cut = pl.ds(lane, LANES)
                outb[b, at, cut] = (run[b, at, cut] * tall * gain[:, lane:lane + LANES]).astype(outb.dtype)
        return 0
    lax.fori_loop(0, batch, fourth, 0)

    def finish(b, _):
        def sent(peer, _):
            time_copy(b, peer).wait_send()
            return 0
        lax.fori_loop(t + 1, times, sent, 0)
        for step in range(1, chans):
            chan_copy(b, step).wait_send()
        return 0
    lax.fori_loop(0, batch, finish, 0)


def shards(decay_rate, drive_in, gate_in, norm_gain):
    times, chans = lax.axis_size("time"), lax.axis_size("chan")
    batch, length, width = decay_rate.shape
    blocks = length // BLOCK
    any_space = pl.BlockSpec(memory_space=pl.ANY)
    vmem = pl.BlockSpec(memory_space=pltpu.VMEM)
    dma = pltpu.SemaphoreType.DMA
    f32 = jnp.float32
    return pl.pallas_call(
        functools.partial(kernel, times, chans),
        out_shape=pltpu.VMEM(decay_rate.shape, jnp.bfloat16),
        in_specs=[any_space] * 4,
        out_specs=vmem,
        scratch_shapes=[
            pltpu.VMEM((width,), f32),
            pltpu.VMEM((BLOCK, 2 * BLOCK), jnp.bfloat16),
            pltpu.VMEM((batch, length, width), f32),
            pltpu.VMEM((batch, length, width), drive_in.dtype),
            pltpu.VMEM((batch, length, width), gate_in.dtype),
            pltpu.VMEM((batch, length, width), f32),
            pltpu.VMEM((batch, blocks, 1, width), f32),
            pltpu.VMEM((batch, blocks, 1, width), f32),
            pltpu.VMEM((batch, 2, width), f32),
            pltpu.VMEM((batch, times, 2, width), f32),
            pltpu.VMEM((length, 2 * LANES), jnp.bfloat16),
            pltpu.VMEM((batch, 1, length), f32),
            pltpu.VMEM((batch, chans - 1, 1, length), f32),
            dma((3, batch)),
            dma((2, blocks)),
            dma,
            dma((batch, times)),
            dma((batch, times)),
            dma((batch, chans - 1)),
            dma((batch, chans - 1)),
        ],
        compiler_params=pltpu.CompilerParams(
            collective_id=0, has_side_effects=True, vmem_limit_bytes=58 * 2 ** 20),
    )(decay_rate, drive_in, gate_in, norm_gain)


def solution(mesh):
    placed = (P(None, "time", "chan"), P(None, "time", "chan"), P(None, "time", "chan"), P("chan"))
    return jax.shard_map(
        shards, mesh=mesh, in_specs=placed, out_specs=P(None, "time", "chan"), check_vma=False
    )
```

```python
import functools
import math

import jax
import jax.numpy as jnp
from jax import lax
from jax.experimental import pallas as pl
from jax.experimental.pallas import tpu as pltpu
from jax.sharding import PartitionSpec as P

BLOCK = 128
LANES = 128
PIECE = 64
MESH = pl.DeviceIdType.MESH


def split(x):
    hi = x.astype(jnp.bfloat16)
    lo = (x - hi.astype(jnp.float32)).astype(jnp.bfloat16)
    return jnp.concatenate([hi, lo], axis=0)


def kernel(times, chans, dec_hbm, drv_hbm, gate_hbm, gain_hbm, outb,
           gain_ref, tri_ref, dec, drv, gate, run, keeps, sums, mine, theirs, folds, power, powers,
           in_sem, head_sem, gain_sem, t_send, t_recv, c_send, c_recv):
    batch, length, width = dec.shape
    blocks = length // BLOCK
    total = length * times
    rate = math.log2(math.e) / total
    scale = 0.5 * total ** -0.5
    t, c = lax.axis_index("time"), lax.axis_index("chan")

    places = ((dec_hbm, dec), (drv_hbm, drv), (gate_hbm, gate))

    def load(i, b):
        return pltpu.make_async_copy(places[i][0].at[b], places[i][1].at[b], in_sem.at[i, b])

    def time_copy(b, peer):
        return pltpu.make_async_remote_copy(
            src_ref=mine.at[b], dst_ref=theirs.at[b, t], send_sem=t_send.at[b, peer],
            recv_sem=t_recv.at[b, t], device_id={"time": peer}, device_id_type=MESH)

    def time_arrival(b, peer):
        return pltpu.make_async_remote_copy(
            src_ref=mine.at[b], dst_ref=theirs.at[b, peer], send_sem=t_send.at[b, peer],
            recv_sem=t_recv.at[b, peer], device_id={"time": peer}, device_id_type=MESH)

    def chan_copy(b, step):
        return pltpu.make_async_remote_copy(
            src_ref=power.at[b], dst_ref=powers.at[b, step - 1], send_sem=c_send.at[b, step - 1],
            recv_sem=c_recv.at[b, step - 1], device_id={"chan": lax.rem(c + step, chans)},
            device_id_type=MESH)

    def head(i, k):
        at = pl.ds(k * BLOCK, BLOCK)
        return pltpu.make_async_copy(
            places[i][0].at[0, at], places[i][1].at[0, at], head_sem.at[i, k])

    for k in range(blocks):
        head(0, k).start()
        head(1, k).start()
    if batch > 1:
        load(0, 1).start()
        load(1, 1).start()

    barrier = pltpu.get_barrier_semaphore()
    for step in range(1, times):
        pl.semaphore_signal(barrier, inc=1, device_id={"time": lax.rem(t + step, times)},
                            device_id_type=MESH)
    for step in range(1, chans):
        pl.semaphore_signal(barrier, inc=1, device_id={"chan": lax.rem(c + step, chans)},
                            device_id_type=MESH)

    below = lax.broadcasted_iota(jnp.int32, (BLOCK, BLOCK), 0) >= lax.broadcasted_iota(
        jnp.int32, (BLOCK, BLOCK), 1)
    lower = jnp.where(below, 1.0, 0.0).astype(jnp.bfloat16)
    tri_ref[:, :BLOCK] = lower
    tri_ref[:, BLOCK:] = lower

    def rows(k):
        return pl.ds(pl.multiple_of(k * BLOCK, BLOCK), BLOCK)

    def first(b, early):
        if not early:
            load(0, b).wait()
            load(1, b).wait()

        def block(k, carried):
            if early:
                head(0, k).wait()
                head(1, k).wait()
            kept, state = carried
            at = rows(k)
            so_far = rate * jnp.dot(tri_ref[...], split(dec[b, at, :]),
                                    preferred_element_type=jnp.float32)
            entered = jnp.exp2(so_far) * drv[b, at, :].astype(jnp.float32)
            dec[b, at, :] = so_far
            run[b, at, :] = entered
            keep = jnp.exp2(-so_far[BLOCK - 1:, :])
            gained = jnp.sum(entered, axis=0, keepdims=True)
            keeps[b, k] = keep
            sums[b, k] = gained
            return kept * keep, keep * (state + gained)

        kept, state = lax.fori_loop(
            0, blocks, block, (jnp.ones((1, width), jnp.float32), jnp.zeros((1, width), jnp.float32)), unroll=2)
        mine[b, 0:1, :] = kept
        mine[b, 1:2, :] = state

    def send_times(b):
        def send(peer, _):
            time_copy(b, peer).start()
            return 0
        lax.fori_loop(t + 1, times, send, 0)

    for b in range(2, batch):
        load(0, b).start()
        load(1, b).start()
    first(0, True)
    for b in range(batch):
        load(2, b).start()
    gain_copy = pltpu.make_async_copy(gain_hbm, gain_ref, gain_sem)
    gain_copy.start()
    pl.semaphore_wait(barrier, times + chans - 2)
    send_times(0)

    def more(b, _):
        first(b, False)
        send_times(b)
        return 0
    lax.fori_loop(1, batch, more, 0)

    def second(b):
        load(2, b).wait()

        def opening(k, _):
            at = pl.ds(pl.multiple_of(k * PIECE, PIECE), PIECE)
            opened = 1.0 + jnp.tanh(0.5 * gate[b, at, :].astype(jnp.float32))
            dec[b, at, :] = jnp.exp2(-dec[b, at, :]) * opened
            return 0
        lax.fori_loop(0, length // PIECE, opening, 0)

        def block(k, _):
            at = rows(k)
            run[b, at, :] = jnp.dot(tri_ref[...], split(run[b, at, :]),
                                    preferred_element_type=jnp.float32)
            return 0
        lax.fori_loop(0, blocks, block, 0, unroll=2)

    def third(b):
        def arrive(peer, state):
            time_arrival(b, peer).wait_recv()
            return theirs[b, peer, 0:1, :] * state + theirs[b, peer, 1:2, :]
        state = lax.fori_loop(0, t, arrive, jnp.zeros((1, width), jnp.float32))

        def block(k, state):
            at = rows(k)
            gated = dec[b, at, :] * (run[b, at, :] + state)
            run[b, at, :] = gated
            squares = gated * gated
            folded = squares[:, :LANES]
            for lane in range(LANES, width, LANES):
                folded = folded + squares[:, lane:lane + LANES]
            hi = folded.astype(jnp.bfloat16)
            folds[at, :LANES] = hi
            folds[at, LANES:] = (folded - hi.astype(jnp.float32)).astype(jnp.bfloat16)
            return keeps[b, k] * (state + sums[b, k])
        lax.fori_loop(0, blocks, block, state)
        power[b] = lax.dot_general(
            jnp.ones((8, 2 * LANES), jnp.bfloat16), folds[...], (((1,), (1,)), ((), ())),
            preferred_element_type=jnp.float32)[0:1]
        for step in range(1, chans):
            chan_copy(b, step).start()

    second(0)

    def middle(b, _):
        second(b)
        third(b - 1)
        return 0
    lax.fori_loop(1, batch, middle, 0)
    third(batch - 1)
    gain_copy.wait()

    def fourth(b, _):
        mean = power[b]
        for step in range(1, chans):
            chan_copy(b, step).wait_recv()
            mean = mean + powers[b, step - 1]
        mean = mean * (scale * scale / (width * chans))
        factor = scale * lax.rsqrt(mean + 1e-6)
        gain = gain_ref[...].reshape(1, width)
        for k in range(blocks):
            at = pl.ds(k * BLOCK, BLOCK)
            tall = jnp.transpose(jnp.broadcast_to(factor[:, k * BLOCK:(k + 1) * BLOCK], (LANES, BLOCK)))
            for lane in range(0, width, LANES):
                cut = pl.ds(lane, LANES)
                outb[b, at, cut] = (run[b, at, cut] * tall * gain[:, lane:lane + LANES]).astype(outb.dtype)
        return 0
    lax.fori_loop(0, batch, fourth, 0)

    def finish(b, _):
        def sent(peer, _):
            time_copy(b, peer).wait_send()
            return 0
        lax.fori_loop(t + 1, times, sent, 0)
        for step in range(1, chans):
            chan_copy(b, step).wait_send()
        return 0
    lax.fori_loop(0, batch, finish, 0)


def shards(decay_rate, drive_in, gate_in, norm_gain):
    times, chans = lax.axis_size("time"), lax.axis_size("chan")
    batch, length, width = decay_rate.shape
    blocks = length // BLOCK
    any_space = pl.BlockSpec(memory_space=pl.ANY)
    vmem = pl.BlockSpec(memory_space=pltpu.VMEM)
    dma = pltpu.SemaphoreType.DMA
    f32 = jnp.float32
    return pl.pallas_call(
        functools.partial(kernel, times, chans),
        out_shape=pltpu.VMEM(decay_rate.shape, jnp.bfloat16),
        in_specs=[any_space] * 4,
        out_specs=vmem,
        scratch_shapes=[
            pltpu.VMEM((width,), f32),
            pltpu.VMEM((BLOCK, 2 * BLOCK), jnp.bfloat16),
            pltpu.VMEM((batch, length, width), f32),
            pltpu.VMEM((batch, length, width), drive_in.dtype),
            pltpu.VMEM((batch, length, width), gate_in.dtype),
            pltpu.VMEM((batch, length, width), f32),
            pltpu.VMEM((batch, blocks, 1, width), f32),
            pltpu.VMEM((batch, blocks, 1, width), f32),
            pltpu.VMEM((batch, 2, width), f32),
            pltpu.VMEM((batch, times, 2, width), f32),
            pltpu.VMEM((length, 2 * LANES), jnp.bfloat16),
            pltpu.VMEM((batch, 1, length), f32),
            pltpu.VMEM((batch, chans - 1, 1, length), f32),
            dma((3, batch)),
            dma((2, blocks)),
            dma,
            dma((batch, times)),
            dma((batch, times)),
            dma((batch, chans - 1)),
            dma((batch, chans - 1)),
        ],
        compiler_params=pltpu.CompilerParams(
            collective_id=0, has_side_effects=True, vmem_limit_bytes=58 * 2 ** 20),
    )(decay_rate, drive_in, gate_in, norm_gain)


def solution(mesh):
    placed = (P(None, "time", "chan"), P(None, "time", "chan"), P(None, "time", "chan"), P("chan"))
    return jax.shard_map(
        shards, mesh=mesh, in_specs=placed, out_specs=P(None, "time", "chan"), check_vma=False
    )
```
